32 devices in a mesh: row: 8 (over z, x), col: 4 (over y, core).
Axes of the slice: x: 2, y: 2, z: 4, core: 2. Of those that a mesh axis runs over, the one named last changes fastest.
Arguments:
- eigvecs: float32 [2048, 512], P('row', 'col'), may hold values from -6 to 6
- reflectors: float32 [8, 32, 128, 64], P(None, ('row', 'col')), may hold values from -2 to 2, as said below
- factors: float32 [8, 32, 64, 64], P(None, ('row', 'col')), may hold values from -3 to 3, as said below
- order: int32 [8], replicated, may hold values from 0 to 7, each once
- offsets: int32 [8], replicated, may hold values from 0 to 63
Outputs:
- rotated: float32 [2048, 512], P('row', 'col')
The draws below stay inside these ranges and needn't reach their ends.
Inputs may be any that keep to these rules, and one draw needn't show every extreme that they name: `order`: a permutation of 0 .. 7. Every block map is orthogonal: with V the block of reflectors and T the block of factors, T is upper triangular and T^-1 + T^-T = V^T V. `factors`: upper triangular, paired with reflectors as promised there.
All inputs are finite; a program needn't handle non-finite values.
Results may differ from the reference program's by a relative error of at most 0.0003.
Values sent between devices are 32-bit elements; how exact they have to be, the bound alone decides.
A program may use at most 64 MiB of HBM per device.

```python
import jax
import jax.numpy as jnp
from jax import lax

NB = 64
SWEEPS = 8
NBLK = 32
ORDER = 2048
VECS = 512


def build_pair(key):
    inner_key = jax.random.fold_in(key, 11)
    spread = 0.03
    identity = jnp.eye(NB, dtype=jnp.float32)
    base = jnp.concatenate([identity, -identity], 0)
    noise = jax.random.normal(inner_key, (SWEEPS, NBLK, 2 * NB, NB), jnp.float32) * spread
    householder = base + noise
    gram = jnp.einsum('abik,abil->abkl', householder, householder, precision=lax.Precision.HIGHEST)
    inverse_factor = jnp.triu(gram, 1) + gram * identity * 0.5
    triangle = lax.linalg.triangular_solve(inverse_factor, jnp.broadcast_to(identity, inverse_factor.shape), left_side=True, lower=False)
    return (householder, triangle)


def draw_reflectors(key, part):
    return build_pair(key)[0]


def draw_factors(key, part):
    return build_pair(key)[1]


def with_ends(drawn, own_key, smallest, top_value):
    longest = drawn.shape.index(max(drawn.shape))
    spots = []
    for shift in (0, 1):
        where = [jax.random.randint(jax.random.fold_in(own_key, axis), (), 0, length) for axis, length in enumerate(drawn.shape)]
        where[longest] = (where[longest] + shift) % drawn.shape[longest]
        spots.append(tuple(where))
    return drawn.at[spots[0]].set(smallest).at[spots[1]].set(top_value)


def block_scale(stream_key, extent, cuts, least, largest):
    def one(dim, shards_of):
        heights = jax.random.uniform(jax.random.fold_in(jax.random.fold_in(stream_key, 6), dim), (shards_of,), jnp.float32, least / len(cuts), largest / len(cuts))
        return jnp.repeat(jnp.exp(heights), extent[dim] // shards_of).reshape((-1,) + (1,) * (len(extent) - dim - 1))

    loudness = one(*cuts[0])
    for cut in cuts[1:]:
        loudness = loudness * one(*cut)
    return loudness


def centred(stream_key, extent, scale, limit, split=(), kind=jnp.bfloat16):
    factor_of = block_scale(stream_key, extent, split, -0.22, 0.18) if split else 1.0
    entries = jax.random.normal(stream_key, extent, jnp.float32) * scale * factor_of
    return jnp.minimum(jnp.maximum(entries, -limit), limit).astype(kind)


def setup_inputs(seed: int = 0) -> dict:
    key_list = jax.random.split(jax.random.key(seed), 6)
    return {
        "eigvecs": centred(key_list[0], (ORDER, VECS), 1.0, 6.0, ((0, 8), (1, 4)), jnp.float32),
        "reflectors": draw_reflectors(jax.random.fold_in(key_list[5], 71), 0),
        "factors": draw_factors(jax.random.fold_in(key_list[5], 71), 0),
        "order": jax.random.permutation(key_list[3], SWEEPS).astype(jnp.int32),
        "offsets": with_ends(jax.random.randint(key_list[4], (SWEEPS,), 0, NB), jax.random.fold_in(key_list[4], 1), 0, NB - 1).astype(jnp.int32),
    }


highest = lax.Precision.HIGHEST

def reflect(segment, householder, triangle):
    inner = jnp.dot(householder.T.astype(jnp.float32), segment.astype(jnp.float32), precision=highest, preferred_element_type=jnp.float32)
    inner = jnp.dot(triangle.astype(jnp.float32), inner.astype(jnp.float32), precision=highest, preferred_element_type=jnp.float32)
    return segment - jnp.dot(householder.astype(jnp.float32), inner.astype(jnp.float32), precision=highest, preferred_element_type=jnp.float32)

def reference(eigvecs, reflectors, factors, order, offsets):
    height = eigvecs.shape[0]
    columns = eigvecs.shape[1]
    number_blocks = reflectors.shape[1]
    vectors = eigvecs
    for position in range(SWEEPS):
        stored = order[position].astype(jnp.int32)
        offset = offsets[stored].astype(jnp.int32)
        house_set = lax.dynamic_index_in_dim(reflectors, stored, 0, keepdims=False)
        tri_set = lax.dynamic_index_in_dim(factors, stored, 0, keepdims=False)
        padded = jnp.concatenate([vectors, jnp.zeros((2 * NB, columns), jnp.float32)], 0)

        def advance(number, current):
            start = (offset + number * NB).astype(jnp.int32)
            segment = lax.dynamic_slice_in_dim(current, start, 2 * NB, 0)
            householder = lax.dynamic_index_in_dim(house_set, number, 0, keepdims=False)
            triangle = lax.dynamic_index_in_dim(tri_set, number, 0, keepdims=False)
            return lax.dynamic_update_slice_in_dim(current, reflect(segment, householder, triangle), start, 0)
        padded = lax.fori_loop(0, number_blocks, advance, padded)
        vectors = padded[:height]
    return vectors
```

```python
import functools

import jax
import jax.numpy as jnp
from jax import lax
from jax.experimental import pallas as pl
from jax.experimental.pallas import tpu as pltpu
from jax.sharding import PartitionSpec as P

MESH = pl.DeviceIdType.MESH
SKEW = 2
FORWARD_LEAD = 1
APPLY_LEAD = 5
CHUNK = 2


def split(x):
    hi = x.astype(jnp.bfloat16)
    lo = (x - hi.astype(jnp.float32)).astype(jnp.bfloat16)
    return hi, lo


def dot(a, b, dims=((1,), (0,))):
    return lax.dot_general(a, b, (dims, ((), ())), preferred_element_type=jnp.float32)


def product(a, b, dims=((1,), (0,))):
    (a_hi, a_lo), (b_hi, b_lo) = a, b
    return dot(a_hi, b_hi, dims) + (dot(a_hi, b_lo, dims) + dot(a_lo, b_hi, dims))


def shape_of_planes(rows_n, per, sweeps):
    planes = rows_n // 2
    own = 2 * per
    total = rows_n * per
    starts = [0] + [own * g + SKEW for g in range(1, planes)] + [total + sweeps - 1]
    most = 0
    for g in range(planes):
        begin, wide = starts[g], starts[g + 1] - starts[g]
        for u in range(wide + sweeps - 1):
            live = [
                a for a in range(wide)
                if 0 <= u - a < sweeps and 0 <= begin + 2 * a - u < total
            ]
            most = max(most, len(live))
    widest = max(starts[g + 1] - starts[g] for g in range(planes))
    return planes, own, total, widest, most


def kernel(
    rows_n, cols_n, order_ref, off_ref, x_ref, house_ref, tri_ref, out_ref,
    pack, stage, map_hi, map_lo, state, turned, final,
    arrive, beside, send_x, send_y, send_b, send_z,
    tile_send, tile_recv, carry_send, carry_recv, last_send, last_recv,
):
    row, col = lax.axis_index("row"), lax.axis_index("col")
    sweeps, _, width, span = house_ref.shape
    height, columns = x_ref.shape
    per = height // span
    half = columns // 2
    planes, own, total, widest, most = shape_of_planes(rows_n, per, sweeps)
    spare = state.shape[0] - 1
    plane, side = lax.div(row, 2), lax.rem(row, 2)
    pair, core = lax.div(col, 2), lax.rem(col, 2)
    row_x, col_y, col_b = row + 1 - 2 * side, lax.rem(col + cols_n // 2, cols_n), col + 1 - 2 * core
    top, bottom = plane == 0, plane == planes - 1

    def start_of(g):
        return jnp.where(g == 0, 0, own * g + SKEW)

    def end_of(g):
        return jnp.where(g == planes - 1, total + sweeps - 1, own * (g + 1) + SKEW)

    def plane_of(s):
        return jnp.minimum(lax.div(jnp.maximum(s - SKEW, 0), own), planes - 1)

    begin = start_of(plane)
    wide = end_of(plane) - begin
    steps = jnp.where(top, jnp.minimum(2 * wide - 1, wide + sweeps - 1), wide + sweeps - 1)

    def lowest(u):
        return jnp.maximum(
            jnp.maximum(u - (sweeps - 1), 0), lax.div(jnp.maximum(u - begin + 1, 0), 2)
        )

    def highest_of(u):
        return jnp.minimum(jnp.minimum(u, wide - 1), lax.div(total - 1 - begin + u, 2))

    def remote(src, dst, sent, got, to_row, to_col):
        return pltpu.make_async_remote_copy(
            src_ref=src, dst_ref=dst, send_sem=sent, recv_sem=got,
            device_id=(to_row, to_col), device_id_type=MESH,
        )

    barrier = pltpu.get_barrier_semaphore()
    greeted = 2
    for to_col in (col_y, col_b):
        pl.semaphore_signal(barrier, inc=1, device_id=(row, to_col), device_id_type=MESH)
    for far in range(-2, 3):
        for x in range(2):
            to_row = 2 * (plane + far) + x
            valid = (to_row >= 0) & (to_row < rows_n) & (to_row != row)
            greeted = greeted + jnp.where(valid, 1, 0)

            @pl.when(valid)
            def _(to_row=to_row):
                pl.semaphore_signal(barrier, inc=1, device_id=(to_row, col), device_id_type=MESH)

    mine = row * per + pair

    def lay_out(p):
        s = mine + p
        g = plane_of(s)
        a = s - start_of(g)
        stored = order_ref[p]
        shift = off_ref[stored] + width * core
        house = pltpu.roll(house_ref[stored, 0], shift, 1)
        tri = tri_ref[stored, 0].T
        packed = jnp.concatenate([tri[: width // 2], tri[width // 2 :]], 1)

        @pl.when(g == plane)
        def _():
            pack[a, p, core, pl.ds(0, width), :] = house
            pack[a, p, core, pl.ds(width, width // 2), :] = packed

        @pl.when(g != plane)
        def _():
            stage[p, pl.ds(0, width), :] = house
            stage[p, pl.ds(width, width // 2), :] = packed

    for p in range(sweeps):
        lay_out(p)

    def move(p, act):
        s = mine + p
        g = plane_of(s)
        a = s - start_of(g)

        @pl.when(g != plane)
        def _():
            act(remote(
                stage.at[p], pack.at[a, p, core], send_z.at[p], arrive.at[a, p],
                2 * g + side, col,
            ))

    def hand_out(t, h, act, keep):
        tile = row * per + t
        g = plane_of(jnp.maximum(tile - 1, 0))
        slot = tile - start_of(g) + sweeps - 1
        to_row = 2 * g + h

        @pl.when(to_row != row)
        def _():
            act(remote(
                turned.at[t, pl.ds(h * half, half)], state.at[slot],
                tile_send.at[t, h], tile_recv.at[slot], to_row, col,
            ))

        if keep:
            @pl.when(to_row == row)
            def _():
                state[slot] = turned[t, pl.ds(h * half, half), :]

    for t in range(per):
        turned[t] = x_ref[pl.ds(t * span, span), :].T

    @pl.when(bottom)
    def _():
        state[total - begin + sweeps - 1] = jnp.zeros((half, span), jnp.float32)

    pl.semaphore_wait(barrier, greeted)
    for p in range(sweeps):
        move(p, lambda c: c.start())
    for t in range(per):
        for h in range(2):
            hand_out(t, h, lambda c: c.start(), True)

    def route(a, p):
        j = begin + a - p
        home_row = lax.div(j, per)
        same_x = side == lax.rem(home_row, 2)
        same_y = pair == lax.rem(j, per)
        native = lax.div(home_row, 2) == plane
        source = same_x & same_y
        by_x = lax.rem(p, 2) == 0
        waits = jnp.logical_not(source & native)
        to_x = source | (same_x & jnp.logical_not(same_y) & jnp.logical_not(by_x))
        to_y = source | (jnp.logical_not(same_x) & same_y & by_x)
        return waits, to_x, to_y

    def copies(a, p):
        place = pack.at[a, p, core]
        return (
            remote(place, place, send_x.at[a, p], arrive.at[a, p], row_x, col),
            remote(place, place, send_y.at[a, p], arrive.at[a, p], row, col_y),
            remote(place, place, send_b.at[a, p], beside.at[a, p], row, col_b),
        )

    def each(u, act):
        low, high = lowest(u), highest_of(u)

        def one(a, _):
            act(a, u - a)
            return 0

        lax.fori_loop(low, high + 1, one, 0)

    def forward(a, p):
        waits, to_x, to_y = route(a, p)
        by_x, by_y, by_b = copies(a, p)

        @pl.when(waits)
        def _():
            by_x.wait_recv()

        @pl.when(to_x)
        def _():
            by_x.start()

        @pl.when(to_y)
        def _():
            by_y.start()

        by_b.start()

    def settle(a, p):
        _, to_x, to_y = route(a, p)
        by_x, by_y, by_b = copies(a, p)

        @pl.when(to_x)
        def _():
            by_x.wait_send()

        @pl.when(to_y)
        def _():
            by_y.wait_send()

        by_b.wait_send()

    def others(a, p):
        place = pack.at[a, p, 1 - core]
        remote(place, place, send_b.at[a, p], beside.at[a, p], row, col_b).wait_recv()

    lane = lax.broadcasted_iota(jnp.int32, (width, span), 1)
    down = lax.broadcasted_iota(jnp.int32, (span, span), 0)
    across = lax.broadcasted_iota(jnp.int32, (span, span), 1)
    eye = jnp.where(down == across, 1.0, 0.0)

    def tri_of(packed):
        return jnp.concatenate([packed, pltpu.roll(packed, width, 1)], 0)[:, :width]

    def compose(a, p):
        offset = off_ref[order_ref[p]]
        v_a, v_b = pack[a, p, 0, pl.ds(0, width), :], pack[a, p, 1, pl.ds(0, width), :]
        t_a = split(tri_of(pack[a, p, 0, pl.ds(width, width // 2), :]))
        t_b = split(tri_of(pack[a, p, 1, pl.ds(width, width // 2), :]))
        shared = ((lane - offset - width) & (span - 1)) < width
        in_a, in_b = lane >= offset, lane >= offset + width
        s_a, s_b = split(v_a), split(v_b)
        lap = product(split(jnp.where(shared, v_a, 0.0)), s_b, ((1,), (1,)))
        f_b = product(t_b, s_b)
        f_a = product(t_a, s_a)
        e = product(t_a, split(lap))
        ef = product(split(e), split(f_b))
        left = jnp.concatenate([
            jnp.where(in_a, f_a, 0.0) - jnp.where(in_b, ef, 0.0), jnp.where(in_b, f_b, 0.0)
        ], 0)
        right = jnp.concatenate([
            jnp.where(in_a, 0.0, f_a) - jnp.where(in_b, 0.0, ef), jnp.where(in_b, 0.0, f_b)
        ], 0)
        tall = jnp.concatenate([v_a, v_b], 0).T
        inside = down >= jnp.where(across < width, offset, offset + width)
        u = jnp.concatenate([jnp.where(inside, tall, 0.0), jnp.where(inside, 0.0, tall)], 0)
        w = jnp.concatenate([left, right], 1)
        low = product(split(u), split(w))
        unit = jnp.concatenate([
            jnp.concatenate([eye, jnp.zeros_like(eye)], 1),
            jnp.concatenate([jnp.zeros_like(eye), eye], 1),
        ], 0)
        return split(unit - low)

    def form(u):
        low, high = lowest(u), highest_of(u)

        def some(q, _):
            spots = [jnp.minimum(low + q * CHUNK + i, high) for i in range(CHUNK)]
            made = [compose(a, u - a) for a in spots]
            for a, (hi, lo) in zip(spots, made):
                map_hi[a, u - a] = hi
                map_lo[a, u - a] = lo
            return 0

        lax.fori_loop(0, lax.div(high - low + CHUNK, CHUNK), some, 0)

    def carry(p, slot):
        return remote(
            state.at[slot], state.at[sweeps - 1 - p], carry_send.at[p], carry_recv.at[p],
            row + 2, col,
        )

    def finish(a, act, keep):
        j = begin + a - (sweeps - 1)
        to_row = lax.div(j, per)
        t = lax.rem(j, per)
        place = pl.ds(side * half, half)

        @pl.when(to_row != row)
        def _():
            act(remote(
                state.at[a], final.at[t, place], last_send.at[a], last_recv.at[t, side],
                to_row, col,
            ))

        if keep:
            @pl.when(to_row == row)
            def _():
                final[t, place, :] = state[a]

    def lasts(u):
        a = u - (sweeps - 1)
        return (a >= 0) & (a == lowest(u)) & (a <= highest_of(u))

    def passes(u):
        return (highest_of(u) == wide - 1) & (lowest(u) <= wide - 1) & jnp.logical_not(bottom)

    def spills(u):
        p = u - wide + 1
        return passes(u) & (begin + wide - 1 - p == 0) & (p < sweeps - 1)

    def apply(u):
        low, high = lowest(u), highest_of(u)
        tile = begin + u + 1

        @pl.when((u < wide) & (tile < total) & (lax.div(tile, per) != row))
        def _():
            remote(
                state.at[u + sweeps], state.at[u + sweeps], tile_send.at[0, 0],
                tile_recv.at[u + sweeps], row_x, col,
            ).wait_recv()

        @pl.when(top & (u == 0) & (row != 0))
        def _():
            remote(
                state.at[sweeps - 1], state.at[sweeps - 1], tile_send.at[0, 0],
                tile_recv.at[sweeps - 1], row_x, col,
            ).wait_recv()

        @pl.when((low == 0) & jnp.logical_not(top))
        def _():
            carry(u, sweeps - 1 - u).wait_recv()

        def some(count):
            ready = []
            for i in range(count):
                a = low + i
                p = u - a
                x = jnp.concatenate([state[a - p + sweeps - 1], state[a - p + sweeps]], 1)
                ready.append((a, p, x, map_hi[a, p], map_lo[a, p]))
            made = []
            for a, p, x, hi, lo in ready:
                x_hi, x_lo = split(x)
                both = dot(jnp.concatenate([x_hi, x_lo], 0), hi)
                made.append((a, p, both[:half] + (both[half:] + dot(x_hi, lo))))
            for a, p, y in made:
                state[a - p + sweeps - 1] = y[:, :span]
                to = jnp.where(begin + a - p == total - 1, spare, a - p + sweeps)
                state[to] = y[:, span:]

        for count in range(1, most + 1):
            @pl.when(high - low + 1 == count)
            def _(count=count):
                some(count)

        @pl.when(passes(u))
        def _():
            p = u - wide + 1
            carry(p, wide - 1 - p + sweeps).start()

        @pl.when(spills(u))
        def _():
            p = u - wide + 1
            carry(p + 1, wide - 1 - p + sweeps - 1).start()

        @pl.when(lasts(u))
        def _():
            finish(u - (sweeps - 1), lambda c: c.start(), True)

    lead = jnp.minimum(FORWARD_LEAD + APPLY_LEAD * plane, steps)

    def main(v, _):
        @pl.when(v < steps)
        def _():
            each(v, forward)

        w = v - FORWARD_LEAD

        @pl.when((w >= 0) & (w < steps))
        def _():
            each(w, others)
            form(w)

        u = v - lead

        @pl.when(u >= 0)
        def _():
            apply(u)

        return 0

    lax.fori_loop(0, steps + lead, main, 0)

    def drain(u, _):
        each(u, settle)

        @pl.when(passes(u))
        def _():
            p = u - wide + 1
            carry(p, wide - 1 - p + sweeps).wait_send()

        @pl.when(spills(u))
        def _():
            p = u - wide + 1
            carry(p + 1, wide - 1 - p + sweeps - 1).wait_send()

        @pl.when(lasts(u))
        def _():
            finish(u - (sweeps - 1), lambda c: c.wait_send(), False)

        return 0

    lax.fori_loop(0, steps, drain, 0)
    for p in range(sweeps):
        move(p, lambda c: c.wait_send())
    for t in range(per):
        for h in range(2):
            hand_out(t, h, lambda c: c.wait_send(), False)
    for t in range(per):
        g = plane_of(row * per + t + sweeps - 1)
        for h in range(2):
            @pl.when(2 * g + h != row)
            def _(t=t, h=h):
                place = final.at[t, pl.ds(h * half, half)]
                remote(
                    place, place, last_send.at[0], last_recv.at[t, h], row_x, col
                ).wait_recv()

        out_ref[pl.ds(t * span, span), :] = final[t].T


def local(rows_n, cols_n, eigvecs, reflectors, factors, order, offsets):
    sweeps, _, span, width = reflectors.shape
    height, columns = eigvecs.shape
    per = height // span
    _, _, _, widest, _ = shape_of_planes(rows_n, per, sweeps)
    slots = widest + sweeps + 1
    vmem = pl.BlockSpec(memory_space=pltpu.VMEM)
    smem = pl.BlockSpec(memory_space=pltpu.SMEM)
    dma = pltpu.SemaphoreType.DMA
    tall = width + width // 2
    return pl.pallas_call(
        functools.partial(kernel, rows_n, cols_n),
        out_shape=jax.ShapeDtypeStruct((height, columns), jnp.float32),
        in_specs=[smem, smem, vmem, vmem, vmem],
        out_specs=vmem,
        scratch_shapes=[
            pltpu.VMEM((widest, sweeps, 2, tall, span), jnp.float32),
            pltpu.VMEM((sweeps, tall, span), jnp.float32),
            pltpu.VMEM((widest, sweeps, 2 * span, 2 * span), jnp.bfloat16),
            pltpu.VMEM((widest, sweeps, 2 * span, 2 * span), jnp.bfloat16),
            pltpu.VMEM((slots, columns // 2, span), jnp.float32),
            pltpu.VMEM((per, columns, span), jnp.float32),
            pltpu.VMEM((per, columns, span), jnp.float32),
            dma((widest, sweeps)),
            dma((widest, sweeps)),
            dma((widest, sweeps)),
            dma((widest, sweeps)),
            dma((widest, sweeps)),
            dma((sweeps,)),
            dma((per, 2)),
            dma((slots,)),
            dma((sweeps,)),
            dma((sweeps,)),
            dma((widest,)),
            dma((per, 2)),
        ],
        compiler_params=pltpu.CompilerParams(collective_id=0, has_side_effects=True),
    )(order, offsets, eigvecs, jnp.swapaxes(reflectors, 2, 3), factors)


def solution(mesh):
    placed = (
        P("row", "col"),
        P(None, ("row", "col"), None, None),
        P(None, ("row", "col"), None, None),
        P(),
        P(),
    )
    body = functools.partial(local, mesh.shape["row"], mesh.shape["col"])
    return jax.shard_map(
        body, mesh=mesh, in_specs=placed, out_specs=P("row", "col"), check_vma=False
    )
```

```python
import functools

import jax
import jax.numpy as jnp
from jax import lax
from jax.experimental import pallas as pl
from jax.experimental.pallas import tpu as pltpu
from jax.sharding import PartitionSpec as P

MESH = pl.DeviceIdType.MESH
SKEW = 2
FORM_LEAD = 1
APPLY_LEAD = 5
CHUNK = 2


def split(x):
    hi = x.astype(jnp.bfloat16)
    lo = (x - hi.astype(jnp.float32)).astype(jnp.bfloat16)
    return hi, lo


def dot(a, b, dims=((1,), (0,))):
    return lax.dot_general(a, b, (dims, ((), ())), preferred_element_type=jnp.float32)


def product(a, b, dims=((1,), (0,))):
    (a_hi, a_lo), (b_hi, b_lo) = a, b
    return dot(a_hi, b_hi, dims) + (dot(a_hi, b_lo, dims) + dot(a_lo, b_hi, dims))


def shape_of_planes(rows_n, per, sweeps):
    planes = rows_n // 2
    own = 2 * per
    total = rows_n * per
    starts = [0] + [own * g + SKEW for g in range(1, planes)] + [total + sweeps - 1]
    most = count = 0
    for g in range(planes):
        begin, wide = starts[g], starts[g + 1] - starts[g]
        over = max(wide - 1 - (total - 1 - begin), 0)
        deep = min(sweeps, begin + wide) - 1
        count = max(count, (wide - 1) * sweeps + deep - over * (over + 1) // 2 + 1)
        for u in range(wide + sweeps - 1):
            live = [
                a for a in range(wide)
                if 0 <= u - a < sweeps and 0 <= begin + 2 * a - u < total
            ]
            most = max(most, len(live))
    widest = max(starts[g + 1] - starts[g] for g in range(planes))
    return planes, own, total, widest, most, count


def kernel(
    rows_n, cols_n, order_ref, off_ref, x_ref, house_ref, tri_ref, out_ref,
    pack, map_hi, map_lo, state, turned, final,
    arrive, beside, sent, send_z,
    tile_send, tile_recv, carry_send, carry_recv, last_send, last_recv, heard,
):
    row, col = lax.axis_index("row"), lax.axis_index("col")
    sweeps, _, width, span = house_ref.shape
    height, columns = x_ref.shape
    per = height // span
    half = columns // 2
    planes, own, total, widest, most, count = shape_of_planes(rows_n, per, sweeps)
    spare = state.shape[0] - 1
    plane, side = lax.div(row, 2), lax.rem(row, 2)
    pair, core = lax.div(col, 2), lax.rem(col, 2)
    row_x, col_y, col_b = row + 1 - 2 * side, lax.rem(col + cols_n // 2, cols_n), col + 1 - 2 * core
    top, bottom = plane == 0, plane == planes - 1

    def start_of(g):
        return jnp.where(g == 0, 0, own * g + SKEW)

    def end_of(g):
        return jnp.where(g == planes - 1, total + sweeps - 1, own * (g + 1) + SKEW)

    def plane_of(s):
        return jnp.minimum(lax.div(jnp.maximum(s - SKEW, 0), own), planes - 1)

    begin = start_of(plane)
    wide = end_of(plane) - begin
    steps = jnp.where(top, jnp.minimum(2 * wide - 1, wide + sweeps - 1), wide + sweeps - 1)

    def lowest(u):
        return jnp.maximum(
            jnp.maximum(u - (sweeps - 1), 0), lax.div(jnp.maximum(u - begin + 1, 0), 2)
        )

    def highest_of(u):
        return jnp.minimum(jnp.minimum(u, wide - 1), lax.div(total - 1 - begin + u, 2))

    def remote(src, dst, left, got, to_row, to_col):
        return pltpu.make_async_remote_copy(
            src_ref=src, dst_ref=dst, send_sem=left, recv_sem=got,
            device_id=(to_row, to_col), device_id_type=MESH,
        )

    barrier = pltpu.get_barrier_semaphore()
    nearest = ((row, col_b, True), (row_x, col, True), (row, col_y, True),
               (row - 2, col, jnp.logical_not(top)), (row + 2, col, jnp.logical_not(bottom)))

    def greet(flag):
        for to_row, to_col, valid in nearest:
            def one(to_row=to_row, to_col=to_col):
                pl.semaphore_signal(
                    flag, inc=1, device_id=(to_row, to_col), device_id_type=MESH
                )

            if valid is True:
                one()
            else:
                pl.when(valid)(one)

    greeted = 3 + jnp.where(top, 0, 1) + jnp.where(bottom, 0, 1)
    greet(barrier)

    mine = row * per + pair

    def place_of(a, p, first=begin):
        over = jnp.maximum(a - (total - 1 - first), 0)
        return a * sweeps + p - lax.div(over * (over + 1), 2)

    def goes_to(p):
        s = mine + p
        g = plane_of(s)
        return g, s - start_of(g)

    down = lax.broadcasted_iota(jnp.int32, (span, span), 0)
    across = lax.broadcasted_iota(jnp.int32, (span, span), 1)
    eye = jnp.where(down == across, 1.0, 0.0)

    def dense(p):
        stored = order_ref[p]
        house = pltpu.roll(house_ref[stored, 0], off_ref[stored] + width * core, 1)
        scaled = product(split(tri_ref[stored, 0].T), split(house))
        return eye - product(split(house.T), split(scaled))

    def stage(p):
        return count + p

    made = [dense(p) for p in range(sweeps)]
    for p in range(sweeps):
        g, a = goes_to(p)
        pack[jnp.where(g == plane, place_of(a, p), stage(p)), core] = made[p]

    def move(p, act, far):
        g, a = goes_to(p)
        apart = jnp.abs(g - plane)

        @pl.when((apart > 1) if far else (apart == 1))
        def _():
            there = place_of(a, p, start_of(g))
            act(remote(
                pack.at[stage(p), core], pack.at[there, core],
                send_z.at[p], arrive.at[there], 2 * g + side, col,
            ))

    def hand_out(t, h, act, keep):
        tile = row * per + t
        g = plane_of(jnp.maximum(tile - 1, 0))
        slot = tile - start_of(g) + sweeps - 1
        to_row = 2 * g + h

        @pl.when(to_row != row)
        def _():
            act(remote(
                turned.at[t, pl.ds(h * half, half)], state.at[slot],
                tile_send.at[t, h], tile_recv.at[slot], to_row, col,
            ))

        if keep:
            @pl.when(to_row == row)
            def _():
                state[slot] = turned[t, pl.ds(h * half, half), :]

    for t in range(per):
        turned[t] = x_ref[pl.ds(t * span, span), :].T

    @pl.when(bottom)
    def _():
        state[total - begin + sweeps - 1] = jnp.zeros((half, span), jnp.float32)

    pl.semaphore_wait(barrier, greeted)
    greet(heard)
    for p in range(sweeps):
        move(p, lambda c: c.start(), False)

    def reach():
        pl.semaphore_wait(heard, greeted)
        for t in range(per):
            for h in range(2):
                hand_out(t, h, lambda c: c.start(), True)
        for p in range(sweeps):
            move(p, lambda c: c.start(), True)

    def route(a, p):
        j = begin + a - p
        home_row = lax.div(j, per)
        same_x = side == lax.rem(home_row, 2)
        same_y = pair == lax.rem(j, per)
        native = lax.div(home_row, 2) == plane
        by_x = lax.rem(p, 2) == 0
        return same_x, same_y, native, by_x

    def copies(a, p):
        n = place_of(a, p)
        place = pack.at[n, core]
        return (
            remote(place, place, sent.at[n], arrive.at[n], row_x, col),
            remote(place, place, sent.at[n], arrive.at[n], row, col_y),
            remote(place, place, sent.at[n], beside.at[n], row, col_b),
        )

    def each(u, act):
        low, high = lowest(u), highest_of(u)

        def one(a, _):
            act(a, u - a)
            return 0

        lax.fori_loop(low, high + 1, one, 0)

    def spread(own_source):
        def one(a, p):
            same_x, same_y, native, _ = route(a, p)
            chosen = native if own_source else jnp.logical_not(native)

            @pl.when(same_x & same_y & chosen)
            def _():
                by_x, by_y, by_b = copies(a, p)
                if not own_source:
                    by_x.wait_recv()
                by_x.start()
                by_y.start()
                by_b.start()

        return one

    def relay(a, p):
        same_x, same_y, _, first_x = route(a, p)

        @pl.when(same_x != same_y)
        def _():
            by_x, by_y, by_b = copies(a, p)
            by_x.wait_recv()

            @pl.when(same_x & jnp.logical_not(first_x))
            def _():
                by_x.start()

            @pl.when(same_y & first_x)
            def _():
                by_y.start()

            by_b.start()

    def finish_ring(a, p):
        same_x, same_y, _, _ = route(a, p)

        @pl.when(jnp.logical_not(same_x | same_y))
        def _():
            by_x, _, by_b = copies(a, p)
            by_x.wait_recv()
            by_b.start()

    def settle(a, p):
        same_x, same_y, _, first_x = route(a, p)
        onward = (same_x & jnp.logical_not(first_x)) | (same_y & first_x)
        times = 1 + jnp.where(same_x & same_y, 2, jnp.where(onward, 1, 0))
        n = place_of(a, p)
        for k in range(1, 4):
            @pl.when(times == k)
            def _(k=k):
                whole = pack.at[pl.ds(0, k), core]
                remote(whole, whole, sent.at[n], arrive.at[n], row_x, col).wait_send()

    def others(a, p):
        n = place_of(a, p)
        place = pack.at[n, 1 - core]
        remote(place, place, sent.at[n], beside.at[n], row, col_b).wait_recv()

    def compose(a, p):
        offset = off_ref[order_ref[p]]
        first, second = pack[place_of(a, p), 0], pack[place_of(a, p), 1]
        zero = jnp.zeros_like(eye)
        row_0, row_1 = down >= offset, down >= offset + width
        col_0, col_1 = across >= offset, across >= offset + width
        middle = ((across - offset) & (span - 1)) >= width
        both = product(split(jnp.where(middle, first, 0.0)), split(second))
        ahead = jnp.where(col_1, both, first)
        quarters = (
            jnp.where(row_0 & col_0, ahead, eye),
            jnp.where(row_0 & jnp.logical_not(col_1), both, zero),
            jnp.where(
                row_0,
                jnp.where(jnp.logical_not(row_1) & col_1, second, zero),
                jnp.where(col_0, ahead, zero),
            ),
            jnp.where(
                row_1 | col_1, eye, jnp.where(row_0, second, both)
            ),
        )
        return [split(q) for q in quarters]

    def form(u):
        low, high = lowest(u), highest_of(u)

        def some(q, _):
            spots = [jnp.minimum(low + q * CHUNK + i, high) for i in range(CHUNK)]
            made = [compose(a, u - a) for a in spots]
            for a, quarters in zip(spots, made):
                for n, (hi, lo) in enumerate(quarters):
                    part = pl.ds(n // 2 * span, span), pl.ds(n % 2 * span, span)
                    map_hi[place_of(a, u - a), *part] = hi
                    map_lo[place_of(a, u - a), *part] = lo
            return 0

        lax.fori_loop(0, lax.div(high - low + CHUNK, CHUNK), some, 0)

    def carry(p, slot):
        return remote(
            state.at[slot], state.at[sweeps - 1 - p], carry_send.at[p], carry_recv.at[p],
            row + 2, col,
        )

    def finish(a, act, keep):
        j = begin + a - (sweeps - 1)
        to_row = lax.div(j, per)
        t = lax.rem(j, per)
        place = pl.ds(side * half, half)

        @pl.when(to_row != row)
        def _():
            act(remote(
                state.at[a], final.at[t, place], last_send.at[a], last_recv.at[t, side],
                to_row, col,
            ))

        if keep:
            @pl.when(to_row == row)
            def _():
                final[t, place, :] = state[a]

    def lasts(u):
        a = u - (sweeps - 1)
        return (a >= 0) & (a == lowest(u)) & (a <= highest_of(u))

    def passes(u):
        return (highest_of(u) == wide - 1) & (lowest(u) <= wide - 1) & jnp.logical_not(bottom)

    def spills(u):
        p = u - wide + 1
        return passes(u) & (begin + wide - 1 - p == 0) & (p < sweeps - 1)

    def apply(u):
        low, high = lowest(u), highest_of(u)
        tile = begin + u + 1

        @pl.when((u < wide) & (tile < total) & (lax.div(tile, per) != row))
        def _():
            remote(
                state.at[u + sweeps], state.at[u + sweeps], tile_send.at[0, 0],
                tile_recv.at[u + sweeps], row_x, col,
            ).wait_recv()

        @pl.when(top & (u == 0) & (row != 0))
        def _():
            remote(
                state.at[sweeps - 1], state.at[sweeps - 1], tile_send.at[0, 0],
                tile_recv.at[sweeps - 1], row_x, col,
            ).wait_recv()

        @pl.when((low == 0) & jnp.logical_not(top))
        def _():
            carry(u, sweeps - 1 - u).wait_recv()

        def some(live):
            ready = []
            for i in range(live):
                a = low + i
                p = u - a
                x = jnp.concatenate([state[a - p + sweeps - 1], state[a - p + sweeps]], 1)
                n = place_of(a, p)
                ready.append((a, p, x, map_hi[n], map_lo[n]))
            made = []
            for a, p, x, hi, lo in ready:
                x_hi, x_lo = split(x)
                both = dot(jnp.concatenate([x_hi, x_lo], 0), hi)
                made.append((a, p, both[:half] + (both[half:] + dot(x_hi, lo))))
            for a, p, y in made:
                state[a - p + sweeps - 1] = y[:, :span]
                to = jnp.where(begin + a - p == total - 1, spare, a - p + sweeps)
                state[to] = y[:, span:]

        for live in range(1, most + 1):
            @pl.when(high - low + 1 == live)
            def _(live=live):
                some(live)

        @pl.when(passes(u))
        def _():
            p = u - wide + 1
            carry(p, wide - 1 - p + sweeps).start()

        @pl.when(spills(u))
        def _():
            p = u - wide + 1
            carry(p + 1, wide - 1 - p + sweeps - 1).start()

        @pl.when(lasts(u))
        def _():
            finish(u - (sweeps - 1), lambda c: c.start(), True)

    def run(*acts):
        def one(v, _):
            for act in acts:
                each(v, act)
            return 0

        lax.fori_loop(0, steps, one, 0)

    run(spread(True))
    reach()
    run(spread(False))
    run(relay)
    lead = jnp.minimum(FORM_LEAD + APPLY_LEAD * plane, FORM_LEAD + steps)

    def main(v, _):
        @pl.when(v < steps)
        def _():
            each(v, finish_ring)

        w = v - FORM_LEAD

        @pl.when((w >= 0) & (w < steps))
        def _():
            each(w, others)
            form(w)

        u = v - lead

        @pl.when(u >= 0)
        def _():
            apply(u)

        return 0

    lax.fori_loop(0, steps + lead, main, 0)

    def drain(u, _):
        each(u, settle)

        @pl.when(passes(u))
        def _():
            p = u - wide + 1
            carry(p, wide - 1 - p + sweeps).wait_send()

        @pl.when(spills(u))
        def _():
            p = u - wide + 1
            carry(p + 1, wide - 1 - p + sweeps - 1).wait_send()

        @pl.when(lasts(u))
        def _():
            finish(u - (sweeps - 1), lambda c: c.wait_send(), False)

        return 0

    lax.fori_loop(0, steps, drain, 0)
    for p in range(sweeps):
        move(p, lambda c: c.wait_send(), False)
        move(p, lambda c: c.wait_send(), True)
    for t in range(per):
        for h in range(2):
            hand_out(t, h, lambda c: c.wait_send(), False)
    for t in range(per):
        g = plane_of(row * per + t + sweeps - 1)
        for h in range(2):
            @pl.when(2 * g + h != row)
            def _(t=t, h=h):
                place = final.at[t, pl.ds(h * half, half)]
                remote(
                    place, place, last_send.at[0], last_recv.at[t, h], row_x, col
                ).wait_recv()

        out_ref[pl.ds(t * span, span), :] = final[t].T


def local(rows_n, cols_n, eigvecs, reflectors, factors, order, offsets):
    sweeps, _, span, width = reflectors.shape
    height, columns = eigvecs.shape
    per = height // span
    _, _, _, widest, _, count = shape_of_planes(rows_n, per, sweeps)
    slots = widest + sweeps + 1
    vmem = pl.BlockSpec(memory_space=pltpu.VMEM)
    smem = pl.BlockSpec(memory_space=pltpu.SMEM)
    dma = pltpu.SemaphoreType.DMA
    return pl.pallas_call(
        functools.partial(kernel, rows_n, cols_n),
        out_shape=jax.ShapeDtypeStruct((height, columns), jnp.float32),
        in_specs=[smem, smem, vmem, vmem, vmem],
        out_specs=vmem,
        scratch_shapes=[
            pltpu.VMEM((count + sweeps, 2, span, span), jnp.float32),
            pltpu.VMEM((count, 2 * span, 2 * span), jnp.bfloat16),
            pltpu.VMEM((count, 2 * span, 2 * span), jnp.bfloat16),
            pltpu.VMEM((slots, columns // 2, span), jnp.float32),
            pltpu.VMEM((per, columns, span), jnp.float32),
            pltpu.VMEM((per, columns, span), jnp.float32),
            dma((count,)),
            dma((count,)),
            dma((count,)),
            dma((sweeps,)),
            dma((per, 2)),
            dma((slots,)),
            dma((sweeps,)),
            dma((sweeps,)),
            dma((widest,)),
            dma((per, 2)),
            pltpu.SemaphoreType.REGULAR,
        ],
        compiler_params=pltpu.CompilerParams(collective_id=0, has_side_effects=True),
    )(order, offsets, eigvecs, jnp.swapaxes(reflectors, 2, 3), factors)


def solution(mesh):
    placed = (
        P("row", "col"),
        P(None, ("row", "col"), None, None),
        P(None, ("row", "col"), None, None),
        P(),
        P(),
    )
    body = functools.partial(local, mesh.shape["row"], mesh.shape["col"])
    return jax.shard_map(
        body, mesh=mesh, in_specs=placed, out_specs=P("row", "col"), check_vma=False
    )
```

```python
import functools

import jax
import jax.numpy as jnp
from jax import lax
from jax.experimental import pallas as pl
from jax.experimental.pallas import tpu as pltpu
from jax.sharding import PartitionSpec as P

MESH = pl.DeviceIdType.MESH
SKEWS = (0, 1, 2, 3)
APPLY_LEAD = 1
FORM_LAG = 1
STRIP = 32
STRIDE = 2
EARLY = 4


def split(x):
    hi = x.astype(jnp.bfloat16)
    lo = (x - hi.astype(jnp.float32)).astype(jnp.bfloat16)
    return hi, lo


def dot(a, b, dims=((1,), (0,))):
    return lax.dot_general(a, b, (dims, ((), ())), preferred_element_type=jnp.float32)


def product(a, b, dims=((1,), (0,))):
    (a_hi, a_lo), (b_hi, b_lo) = a, b
    return dot(a_hi, b_hi, dims) + (dot(a_hi, b_lo, dims) + dot(a_lo, b_hi, dims))


def shape_of_planes(rows_n, per, sweeps):
    planes = rows_n // 2
    own = 2 * per
    total = rows_n * per
    starts = [0] + [own * g + SKEWS[min(g, len(SKEWS) - 1)] for g in range(1, planes)] + [total + sweeps - 1]
    most = count = 0
    for g in range(planes):
        begin, wide = starts[g], starts[g + 1] - starts[g]
        over = max(wide - 1 - (total - 1 - begin), 0)
        deep = min(sweeps, begin + wide) - 1
        count = max(count, (wide - 1) * sweeps + deep - over * (over + 1) // 2 + 1)
        for u in range(wide + STRIDE * (sweeps - 1)):
            live = [
                p for p in range(sweeps)
                if 0 <= u - STRIDE * p < wide
                and 0 <= begin + u - (STRIDE + 1) * p < total
            ]
            most = max(most, len(live))
    widest = max(starts[g + 1] - starts[g] for g in range(planes))
    return planes, own, total, widest, most, count


def kernel(
    rows_n, cols_n, order_ref, off_ref, x_ref, house_ref, tri_ref, out_ref,
    pack, map_hi, map_lo, state, turned, final,
    arrive, beside, sent, send_z,
    tile_send, tile_recv, carry_send, carry_recv, last_send, last_recv, heard,
):
    row, col = lax.axis_index("row"), lax.axis_index("col")
    sweeps, _, width, span = house_ref.shape
    height, columns = x_ref.shape
    per = height // span
    half = columns // 2
    planes, own, total, widest, most, count = shape_of_planes(rows_n, per, sweeps)
    spare = state.shape[0] - 1
    plane, side = lax.div(row, 2), lax.rem(row, 2)
    pair, core = lax.div(col, 2), lax.rem(col, 2)
    row_x, col_y, col_b = row + 1 - 2 * side, lax.rem(col + cols_n // 2, cols_n), col + 1 - 2 * core
    top, bottom = plane == 0, plane == planes - 1

    def start_of(g):
        skew = SKEWS[-1]
        for n in range(len(SKEWS) - 2, -1, -1):
            skew = jnp.where(g == n, SKEWS[n], skew)
        return own * g + skew

    def end_of(g):
        return jnp.where(g == planes - 1, total + sweeps - 1, start_of(g + 1))

    def plane_of(s):
        g = jnp.minimum(lax.div(s, own), planes - 1)
        return g - jnp.where(s < start_of(g), 1, 0)

    begin = start_of(plane)
    wide = end_of(plane) - begin
    deepest = jnp.where(top, jnp.minimum(sweeps - 1, wide - 1), sweeps - 1)
    steps = wide + STRIDE * deepest

    def window(u):
        def over(x, n):
            return lax.div(jnp.maximum(x, 0) + n - 1, n)

        low = jnp.maximum(over(u - wide + 1, STRIDE), over(begin + u - total + 1, STRIDE + 1))
        high = jnp.minimum(lax.div(u, STRIDE), lax.div(begin + u, STRIDE + 1))
        return low, jnp.minimum(high, sweeps - 1)

    def remote(src, dst, left, got, to_row, to_col):
        return pltpu.make_async_remote_copy(
            src_ref=src, dst_ref=dst, send_sem=left, recv_sem=got,
            device_id=(to_row, to_col), device_id_type=MESH,
        )

    barrier = pltpu.get_barrier_semaphore()
    nearest = ((row, col_b, True), (row_x, col, True), (row, col_y, True),
               (row - 2, col, jnp.logical_not(top)), (row + 2, col, jnp.logical_not(bottom)))

    def greet(flag):
        for to_row, to_col, valid in nearest:
            def one(to_row=to_row, to_col=to_col):
                pl.semaphore_signal(
                    flag, inc=1, device_id=(to_row, to_col), device_id_type=MESH
                )

            if valid is True:
                one()
            else:
                pl.when(valid)(one)

    greeted = 3 + jnp.where(top, 0, 1) + jnp.where(bottom, 0, 1)
    greet(barrier)

    mine = row * per + pair

    def place_of(a, p, first=begin):
        over = jnp.maximum(a - (total - 1 - first), 0)
        return a * sweeps + p - lax.div(over * (over + 1), 2)

    def goes_to(p):
        s = mine + p
        g = plane_of(s)
        return g, s - start_of(g)

    down = lax.broadcasted_iota(jnp.int32, (span, span), 0)
    across = lax.broadcasted_iota(jnp.int32, (span, span), 1)
    eye = jnp.where(down == across, 1.0, 0.0)

    def dense(p):
        stored = order_ref[p]
        house = pltpu.roll(house_ref[stored, 0], off_ref[stored] + width * core, 1)
        scaled = product(split(tri_ref[stored, 0].T), split(house))
        return eye - product(split(house.T), split(scaled))

    def stage(p):
        return count + p

    def prepare(low, high):
        made = [dense(p) for p in range(low, high)]
        for p in range(low, high):
            g, a = goes_to(p)
            pack[jnp.where(g == plane, place_of(a, p), stage(p)), core] = made[p - low]

    def move(p, act, far):
        g, a = goes_to(p)
        apart = jnp.abs(g - plane)

        @pl.when((apart > 1) if far else (apart == 1))
        def _():
            there = place_of(a, p, start_of(g))
            act(remote(
                pack.at[stage(p), core], pack.at[there, core],
                send_z.at[p], arrive.at[there], 2 * g + side, col,
            ))

    def hand_out(t, h, act, keep):
        tile = row * per + t
        g = plane_of(jnp.maximum(tile - 1, 0))
        slot = tile - start_of(g) + sweeps - 1
        to_row = 2 * g + h

        @pl.when(to_row != row)
        def _():
            act(remote(
                turned.at[t, pl.ds(h * half, half)], state.at[slot],
                tile_send.at[t, h], tile_recv.at[slot], to_row, col,
            ))

        if keep:
            @pl.when(to_row == row)
            def _():
                state[slot] = turned[t, pl.ds(h * half, half), :]

    def reach():
        pl.semaphore_wait(heard, greeted)
        for p in range(sweeps):
            move(p, lambda c: c.start(), True)

    kin = per
    most_lines = -(-widest // own)
    here = side * kin + pair
    over_x, over_y = (1 - side) * kin + pair, side * kin + (kin - 1 - pair)
    over_both = (1 - side) * kin + (kin - 1 - pair)

    def copies(a, p):
        n = place_of(a, p)
        place = pack.at[n, core]
        return (
            remote(place, place, sent.at[p], arrive.at[n], row_x, col),
            remote(place, place, sent.at[p], arrive.at[n], row, col_y),
            remote(place, place, sent.at[p], beside.at[n], row, col_b),
            remote(place, place, sent.at[p], arrive.at[n], row_x, col_y),
        )

    def line(which, p):
        low = jnp.maximum(begin - p, 0)
        high = jnp.minimum(begin + wide - 1 - p, total - 1)
        low = low + lax.rem(which - lax.rem(low, own) + own, own)
        return low, lax.div(jnp.maximum(high - low + own, 0), own)

    def kind(which, p, act, skip=0):
        low, many = line(which, p)

        def one(i, _):
            j = low + i * own
            act(j - begin + p, p, j)
            return 0

        lax.fori_loop(skip, many, one, 0)

    def is_native(j):
        return lax.div(j, own) == plane

    def sow(a, p, j):
        native = is_native(j)
        by_x, by_y, by_b, by_both = copies(a, p)

        @pl.when(jnp.logical_not(native))
        def _():
            by_x.wait_recv()

        by_x.start()
        by_y.start()

        @pl.when(direct(j))
        def _():
            by_both.start()

        by_b.start()

    def direct(j):
        return top & jnp.logical_not(is_native(j))

    def only(test, wanted, act):
        def one(a, p, j):
            @pl.when(test(j) if wanted else jnp.logical_not(test(j)))
            def _():
                act(a, p, j)

        return one

    def onward_x(p):
        return lax.rem(p, 2) == 1

    def relay_x(a, p, j):
        by_x, by_y, by_b, _ = copies(a, p)
        by_x.wait_recv()

        @pl.when(jnp.logical_not(onward_x(p) | direct(j)))
        def _():
            by_y.start()

        by_b.start()

    def relay_y(a, p, j):
        by_x, by_y, by_b, _ = copies(a, p)
        by_x.wait_recv()

        @pl.when(onward_x(p) & jnp.logical_not(direct(j)))
        def _():
            by_x.start()

        by_b.start()

    def close(a, p, j):
        by_x, _, by_b, _ = copies(a, p)
        by_x.wait_recv()
        by_b.start()

    def form(*spots):
        places = [(place_of(a, p), p) for a, p in spots]
        for n, _ in places:
            beyond = pack.at[n, 1 - core]
            remote(beyond, beyond, sent.at[0], beside.at[n], row, col_b).wait_recv()
        joint = []
        for n, p in places:
            offset = off_ref[order_ref[p]]
            middle = ((across - offset) & (span - 1)) >= width
            joint.append(
                product(split(jnp.where(middle, pack[n, 0], 0.0)), split(pack[n, 1]))
            )
        for (n, p), joined in zip(places, joint):
            offset = off_ref[order_ref[p]]
            for r in range(0, span, STRIP):
                rows = pl.ds(r, STRIP)
                down_r = r + lax.broadcasted_iota(jnp.int32, (STRIP, span), 0)
                across_r = lax.broadcasted_iota(jnp.int32, (STRIP, span), 1)
                unit = jnp.where(down_r == across_r, 1.0, 0.0)
                row_0, row_1 = down_r >= offset, down_r >= offset + width
                col_0, col_1 = across_r >= offset, across_r >= offset + width
                first, second = pack[n, 0, rows, :], pack[n, 1, rows, :]
                both = joined[r : r + STRIP]
                ahead = jnp.where(col_1, both, first)
                quarters = (
                    jnp.where(row_0 & col_0, ahead, unit),
                    jnp.where(row_0 & jnp.logical_not(col_1), both, 0.0),
                    jnp.where(
                        row_0,
                        jnp.where(jnp.logical_not(row_1) & col_1, second, 0.0),
                        jnp.where(col_0, ahead, 0.0),
                    ),
                    jnp.where(row_1 | col_1, unit, jnp.where(row_0, second, both)),
                )
                for q, quarter in enumerate(quarters):
                    hi, lo = split(quarter)
                    part = pl.ds(q // 2 * span + r, STRIP), pl.ds(q % 2 * span, span)
                    map_hi[n, *part] = hi
                    map_lo[n, *part] = lo

    def form_one(a, p, j):
        form((a, p))

    def form_near(p):
        lines = [line(which, p) for which in (here, over_x, over_y)]
        full = True
        for low, many in lines:
            full = full & (many > 0) & jnp.logical_not(direct(low))

        @pl.when(full)
        def _():
            form(*[(low - begin + p, p) for low, _ in lines])

        skip = jnp.where(full, 1, 0)
        for which in (here, over_x, over_y):
            kind(which, p, only(direct, False, form_one), skip)

    def carry(p, slot):
        return remote(
            state.at[slot], state.at[sweeps - 1 - p], carry_send.at[p], carry_recv.at[p],
            row + 2, col,
        )

    def finish(a, act, keep):
        j = begin + a - (sweeps - 1)
        to_row = lax.div(j, per)
        t = lax.rem(j, per)
        place = pl.ds(side * half, half)

        @pl.when(to_row != row)
        def _():
            act(remote(
                state.at[a], final.at[t, place], last_send.at[a], last_recv.at[t, side],
                to_row, col,
            ))

        if keep:
            @pl.when(to_row == row)
            def _():
                final[t, place, :] = state[a]

    def lasts(u):
        low, high = window(u)
        return (high == sweeps - 1) & (low <= high)

    def passes(u):
        low, high = window(u)
        return (u - STRIDE * low == wide - 1) & (low <= high) & jnp.logical_not(bottom)

    def spills(u):
        p = window(u)[0]
        return passes(u) & (begin + wide - 1 - p == 0) & (p < sweeps - 1)

    def apply(u):
        low, high = window(u)
        tile = begin + u + 1

        @pl.when((u < wide) & (tile < total) & (lax.div(tile, per) != row))
        def _():
            remote(
                state.at[u + sweeps], state.at[u + sweeps], tile_send.at[0, 0],
                tile_recv.at[u + sweeps], row_x, col,
            ).wait_recv()

        @pl.when(top & (u == 0) & (row != 0))
        def _():
            remote(
                state.at[sweeps - 1], state.at[sweeps - 1], tile_send.at[0, 0],
                tile_recv.at[sweeps - 1], row_x, col,
            ).wait_recv()

        @pl.when((u == STRIDE * high) & (low <= high) & jnp.logical_not(top))
        def _():
            carry(high, sweeps - 1 - high).wait_recv()

        def some(live):
            ready = []
            for i in range(live):
                p = low + i
                a = u - STRIDE * p
                x = jnp.concatenate([state[a - p + sweeps - 1], state[a - p + sweeps]], 1)
                n = place_of(a, p)
                ready.append((a, p, x, map_hi[n], map_lo[n]))
            made = []
            for a, p, x, hi, lo in ready:
                x_hi, x_lo = split(x)
                both = dot(jnp.concatenate([x_hi, x_lo], 0), hi)
                made.append((a, p, both[:half] + (both[half:] + dot(x_hi, lo))))
            for a, p, y in made:
                state[a - p + sweeps - 1] = y[:, :span]
                to = jnp.where(begin + a - p == total - 1, spare, a - p + sweeps)
                state[to] = y[:, span:]

        for live in range(1, most + 1):
            @pl.when(high - low + 1 == live)
            def _(live=live):
                some(live)

        @pl.when(passes(u))
        def _():
            p = window(u)[0]
            carry(p, wide - 1 - p + sweeps).start()

        @pl.when(spills(u))
        def _():
            p = window(u)[0]
            carry(p + 1, wide - 1 - p + sweeps - 1).start()

        @pl.when(lasts(u))
        def _():
            finish(u - STRIDE * (sweeps - 1), lambda c: c.start(), True)

    def over_sweeps(act):
        def one(p, _):
            act(p)
            return 0

        lax.fori_loop(0, sweeps, one, 0)

    def turn(v):
        return v

    def near(v, _):
        @pl.when(v < sweeps)
        def _():
            kind(over_x, turn(v), only(direct, False, relay_x))
            kind(over_y, turn(v), only(direct, False, relay_y))

        p = v - FORM_LAG

        @pl.when(p >= 0)
        def _():
            form_near(turn(p))

        return 0

    def drain_maps(p):
        lines = [line(which, p)[1] for which in (here, over_x, over_y, over_both)]
        straight = [jnp.where(top, jnp.maximum(many - 1, 0), 0) for many in lines]
        turns = jnp.where(onward_x(p), 1, 0)
        total_sends = (
            3 * lines[0] + straight[0] + lines[3]
            + lines[1] + (1 - turns) * (lines[1] - straight[1])
            + lines[2] + turns * (lines[2] - straight[2])
        )
        for k in range(1, 3 * most_lines + 5 * most_lines + 1):
            @pl.when(total_sends == k)
            def _(k=k):
                whole = pack.at[pl.ds(0, k), core]
                remote(whole, whole, sent.at[p], arrive.at[0], row_x, col).wait_send()

    def main(v, _):
        @pl.when(v < sweeps)
        def _():
            kind(over_both, v, close)

            @pl.when(top)
            def _():
                kind(over_x, v, only(direct, True, close))
                kind(over_y, v, only(direct, True, close))

        p = v - FORM_LAG

        @pl.when((p >= 0) & (p < sweeps))
        def _():
            kind(over_both, p, form_one)

            @pl.when(top)
            def _():
                for which in (here, over_x, over_y):
                    kind(which, p, only(direct, True, form_one))

        @pl.when((v == sweeps + FORM_LAG) & (plane > 1))
        def _():
            over_sweeps(drain_maps)

        def one(k, _):
            u = (v - lead) * STRIDE + k

            @pl.when((u >= 0) & (u < steps))
            def _():
                apply(u)

            return 0

        lax.fori_loop(0, STRIDE, one, 0)
        return 0

    def begin_sweeps(low, high):
        for p in range(low, high):
            move(p, lambda c: c.start(), False)

        def one(p, _):
            kind(here, p, only(is_native, True, sow))
            return 0

        lax.fori_loop(low, high, one, 0)

    prepare(0, EARLY)
    pl.semaphore_wait(barrier, greeted)
    greet(heard)
    begin_sweeps(0, EARLY)
    prepare(EARLY, sweeps)
    begin_sweeps(EARLY, sweeps)
    for t in range(per):
        turned[t] = x_ref[pl.ds(t * span, span), :].T

    @pl.when(bottom)
    def _():
        state[total - begin + sweeps - 1] = jnp.zeros((half, span), jnp.float32)


    reach()
    over_sweeps(lambda p: kind(here, p, only(is_native, False, sow)))
    for t in range(per):
        for h in range(2):
            hand_out(t, h, lambda c: c.start(), True)
    lax.fori_loop(0, sweeps + FORM_LAG, near, 0)
    lead = FORM_LAG + jnp.where(top, 0, jnp.where(plane == 1, APPLY_LEAD, sweeps))
    lax.fori_loop(
        0, jnp.maximum(sweeps + FORM_LAG + 1, lax.div(steps + STRIDE - 1, STRIDE) + lead), main, 0
    )

    def drain(u, _):

        @pl.when(passes(u))
        def _():
            p = window(u)[0]
            carry(p, wide - 1 - p + sweeps).wait_send()

        @pl.when(spills(u))
        def _():
            p = window(u)[0]
            carry(p + 1, wide - 1 - p + sweeps - 1).wait_send()

        @pl.when(lasts(u))
        def _():
            finish(u - STRIDE * (sweeps - 1), lambda c: c.wait_send(), False)

        return 0

    lax.fori_loop(0, steps, drain, 0)

    @pl.when(plane <= 1)
    def _():
        over_sweeps(drain_maps)

    for p in range(sweeps):
        move(p, lambda c: c.wait_send(), False)
        move(p, lambda c: c.wait_send(), True)
    for t in range(per):
        for h in range(2):
            hand_out(t, h, lambda c: c.wait_send(), False)
    for t in range(per):
        g = plane_of(row * per + t + sweeps - 1)
        for h in range(2):
            @pl.when(2 * g + h != row)
            def _(t=t, h=h):
                place = final.at[t, pl.ds(h * half, half)]
                remote(
                    place, place, last_send.at[0], last_recv.at[t, h], row_x, col
                ).wait_recv()

        out_ref[pl.ds(t * span, span), :] = final[t].T


def local(rows_n, cols_n, eigvecs, reflectors, factors, order, offsets):
    sweeps, _, span, width = reflectors.shape
    height, columns = eigvecs.shape
    per = height // span
    _, _, _, widest, _, count = shape_of_planes(rows_n, per, sweeps)
    slots = widest + sweeps + 1
    vmem = pl.BlockSpec(memory_space=pltpu.VMEM)
    smem = pl.BlockSpec(memory_space=pltpu.SMEM)
    dma = pltpu.SemaphoreType.DMA
    return pl.pallas_call(
        functools.partial(kernel, rows_n, cols_n),
        out_shape=jax.ShapeDtypeStruct((height, columns), jnp.float32),
        in_specs=[smem, smem, vmem, vmem, vmem],
        out_specs=vmem,
        scratch_shapes=[
            pltpu.VMEM((count + sweeps, 2, span, span), jnp.float32),
            pltpu.VMEM((count, 2 * span, 2 * span), jnp.bfloat16),
            pltpu.VMEM((count, 2 * span, 2 * span), jnp.bfloat16),
            pltpu.VMEM((slots, columns // 2, span), jnp.float32),
            pltpu.VMEM((per, columns, span), jnp.float32),
            pltpu.VMEM((per, columns, span), jnp.float32),
            dma((count,)),
            dma((count,)),
            dma((sweeps,)),
            dma((sweeps,)),
            dma((per, 2)),
            dma((slots,)),
            dma((sweeps,)),
            dma((sweeps,)),
            dma((widest,)),
            dma((per, 2)),
            pltpu.SemaphoreType.REGULAR,
        ],
        compiler_params=pltpu.CompilerParams(collective_id=0, has_side_effects=True),
    )(order, offsets, eigvecs, jnp.swapaxes(reflectors, 2, 3), factors)


def solution(mesh):
    placed = (
        P("row", "col"),
        P(None, ("row", "col"), None, None),
        P(None, ("row", "col"), None, None),
        P(),
        P(),
    )
    body = functools.partial(local, mesh.shape["row"], mesh.shape["col"])
    return jax.shard_map(
        body, mesh=mesh, in_specs=placed, out_specs=P("row", "col"), check_vma=False
    )
```

```python
import functools

import jax
import jax.numpy as jnp
from jax import lax
from jax.experimental import pallas as pl
from jax.experimental.pallas import tpu as pltpu
from jax.sharding import PartitionSpec as P

MESH = pl.DeviceIdType.MESH
SKEWS = (0, 1, 2, 3)
APPLY_LEAD = 1
FORM_LAG = 1
STRIP = 32
STRIDE = 2
EARLY = 2


def split(x):
    hi = x.astype(jnp.bfloat16)
    lo = (x - hi.astype(jnp.float32)).astype(jnp.bfloat16)
    return hi, lo


def dot(a, b, dims=((1,), (0,))):
    return lax.dot_general(a, b, (dims, ((), ())), preferred_element_type=jnp.float32)


def product(a, b, dims=((1,), (0,))):
    (a_hi, a_lo), (b_hi, b_lo) = a, b
    return dot(a_hi, b_hi, dims) + (dot(a_hi, b_lo, dims) + dot(a_lo, b_hi, dims))


def shape_of_planes(rows_n, per, sweeps):
    planes = rows_n // 2
    own = 2 * per
    total = rows_n * per
    starts = [0] + [own * g + SKEWS[min(g, len(SKEWS) - 1)] for g in range(1, planes)] + [total + sweeps - 1]
    most = count = 0
    for g in range(planes):
        begin, wide = starts[g], starts[g + 1] - starts[g]
        over = max(wide - 1 - (total - 1 - begin), 0)
        deep = min(sweeps, begin + wide) - 1
        count = max(count, (wide - 1) * sweeps + deep - over * (over + 1) // 2 + 1)
        for u in range(wide + STRIDE * (sweeps - 1)):
            live = [
                p for p in range(sweeps)
                if 0 <= u - STRIDE * p < wide
                and 0 <= begin + u - (STRIDE + 1) * p < total
            ]
            most = max(most, len(live))
    widest = max(starts[g + 1] - starts[g] for g in range(planes))
    return planes, own, total, widest, most, count


def kernel(
    rows_n, cols_n, order_ref, off_ref, x_hbm, house_hbm, tri_hbm, out_ref,
    x_ref, house_ref, tri_ref, load_sem,
    pack, map_hi, map_lo, state, turned, final,
    arrive, beside, sent, send_z,
    tile_send, tile_recv, carry_send, carry_recv, last_send, last_recv, heard,
):
    row, col = lax.axis_index("row"), lax.axis_index("col")
    sweeps, _, width, span = house_ref.shape
    height, columns = x_ref.shape
    per = height // span
    half = columns // 2
    planes, own, total, widest, most, count = shape_of_planes(rows_n, per, sweeps)
    spare = state.shape[0] - 1
    plane, side = lax.div(row, 2), lax.rem(row, 2)
    pair, core = lax.div(col, 2), lax.rem(col, 2)
    row_x, col_y, col_b = row + 1 - 2 * side, lax.rem(col + cols_n // 2, cols_n), col + 1 - 2 * core
    top, bottom = plane == 0, plane == planes - 1

    def start_of(g):
        skew = SKEWS[-1]
        for n in range(len(SKEWS) - 2, -1, -1):
            skew = jnp.where(g == n, SKEWS[n], skew)
        return own * g + skew

    def end_of(g):
        return jnp.where(g == planes - 1, total + sweeps - 1, start_of(g + 1))

    def plane_of(s):
        g = jnp.minimum(lax.div(s, own), planes - 1)
        return g - jnp.where(s < start_of(g), 1, 0)

    begin = start_of(plane)
    wide = end_of(plane) - begin
    deepest = jnp.where(top, jnp.minimum(sweeps - 1, wide - 1), sweeps - 1)
    steps = wide + STRIDE * deepest

    def window(u):
        def over(x, n):
            return lax.div(jnp.maximum(x, 0) + n - 1, n)

        low = jnp.maximum(over(u - wide + 1, STRIDE), over(begin + u - total + 1, STRIDE + 1))
        high = jnp.minimum(lax.div(u, STRIDE), lax.div(begin + u, STRIDE + 1))
        return low, jnp.minimum(high, sweeps - 1)

    def remote(src, dst, left, got, to_row, to_col):
        return pltpu.make_async_remote_copy(
            src_ref=src, dst_ref=dst, send_sem=left, recv_sem=got,
            device_id=(to_row, to_col), device_id_type=MESH,
        )

    loads = [
        pltpu.make_async_copy(src, dst, load_sem.at[n])
        for n, (src, dst) in enumerate(
            ((house_hbm, house_ref), (tri_hbm, tri_ref), (x_hbm, x_ref))
        )
    ]
    for load in loads:
        load.start()
    barrier = pltpu.get_barrier_semaphore()
    nearest = ((row, col_b, True), (row_x, col, True), (row, col_y, True),
               (row - 2, col, jnp.logical_not(top)), (row + 2, col, jnp.logical_not(bottom)))

    def greet(flag):
        for to_row, to_col, valid in nearest:
            def one(to_row=to_row, to_col=to_col):
                pl.semaphore_signal(
                    flag, inc=1, device_id=(to_row, to_col), device_id_type=MESH
                )

            if valid is True:
                one()
            else:
                pl.when(valid)(one)

    greeted = 3 + jnp.where(top, 0, 1) + jnp.where(bottom, 0, 1)
    greet(barrier)

    mine = row * per + pair

    def place_of(a, p, first=begin):
        over = jnp.maximum(a - (total - 1 - first), 0)
        return a * sweeps + p - lax.div(over * (over + 1), 2)

    def goes_to(p):
        s = mine + p
        g = plane_of(s)
        return g, s - start_of(g)

    down = lax.broadcasted_iota(jnp.int32, (span, span), 0)
    across = lax.broadcasted_iota(jnp.int32, (span, span), 1)
    eye = jnp.where(down == across, 1.0, 0.0)

    def dense(p):
        stored = order_ref[p]
        house = pltpu.roll(house_ref[stored, 0], off_ref[stored] + width * core, 1)
        scaled = product(split(tri_ref[stored, 0].T), split(house))
        return eye - product(split(house.T), split(scaled))

    def stage(p):
        return count + p

    def prepare(low, high):
        made = [dense(p) for p in range(low, high)]
        for p in range(low, high):
            g, a = goes_to(p)
            pack[jnp.where(g == plane, place_of(a, p), stage(p)), core] = made[p - low]

    def move(p, act, far):
        g, a = goes_to(p)
        apart = jnp.abs(g - plane)

        @pl.when((apart > 1) if far else (apart == 1))
        def _():
            there = place_of(a, p, start_of(g))
            act(remote(
                pack.at[stage(p), core], pack.at[there, core],
                send_z.at[p], arrive.at[there], 2 * g + side, col,
            ))

    def hand_out(t, h, act, keep):
        tile = row * per + t
        g = plane_of(jnp.maximum(tile - 1, 0))
        slot = tile - start_of(g) + sweeps - 1
        to_row = 2 * g + h

        @pl.when(to_row != row)
        def _():
            act(remote(
                turned.at[t, pl.ds(h * half, half)], state.at[slot],
                tile_send.at[t, h], tile_recv.at[slot - sweeps + 1], to_row, col,
            ))

        if keep:
            @pl.when(to_row == row)
            def _():
                state[slot] = turned[t, pl.ds(h * half, half), :]

    def reach():
        pl.semaphore_wait(heard, greeted)
        for p in range(sweeps):
            move(p, lambda c: c.start(), True)

    kin = per
    most_lines = -(-widest // own)
    here = side * kin + pair
    over_x, over_y = (1 - side) * kin + pair, side * kin + (kin - 1 - pair)
    over_both = (1 - side) * kin + (kin - 1 - pair)

    def copies(a, p):
        n = place_of(a, p)
        place = pack.at[n, core]
        return (
            remote(place, place, sent.at[p], arrive.at[n], row_x, col),
            remote(place, place, sent.at[p], arrive.at[n], row, col_y),
            remote(place, place, sent.at[p], beside.at[n], row, col_b),
            remote(place, place, sent.at[p], arrive.at[n], row_x, col_y),
        )

    def line(which, p):
        low = jnp.maximum(begin - p, 0)
        high = jnp.minimum(begin + wide - 1 - p, total - 1)
        low = low + lax.rem(which - lax.rem(low, own) + own, own)
        return low, lax.div(jnp.maximum(high - low + own, 0), own)

    def kind(which, p, act, skip=0):
        low, many = line(which, p)

        def one(i, _):
            j = low + i * own
            act(j - begin + p, p, j)
            return 0

        lax.fori_loop(skip, many, one, 0)

    def is_native(j):
        return lax.div(j, own) == plane

    def sow(a, p, j):
        native = is_native(j)
        by_x, by_y, by_b, by_both = copies(a, p)

        @pl.when(jnp.logical_not(native))
        def _():
            by_x.wait_recv()

        by_x.start()
        by_y.start()

        @pl.when(direct(j))
        def _():
            by_both.start()

        by_b.start()

    def direct(j):
        return top & jnp.logical_not(is_native(j))

    def only(test, wanted, act):
        def one(a, p, j):
            @pl.when(test(j) if wanted else jnp.logical_not(test(j)))
            def _():
                act(a, p, j)

        return one

    def onward_x(p):
        return lax.rem(p, 2) == 1

    def relay_x(a, p, j):
        by_x, by_y, by_b, _ = copies(a, p)
        by_x.wait_recv()

        @pl.when(jnp.logical_not(onward_x(p) | direct(j)))
        def _():
            by_y.start()

        by_b.start()

    def relay_y(a, p, j):
        by_x, by_y, by_b, _ = copies(a, p)
        by_x.wait_recv()

        @pl.when(onward_x(p) & jnp.logical_not(direct(j)))
        def _():
            by_x.start()

        by_b.start()

    def close(a, p, j):
        by_x, _, by_b, _ = copies(a, p)
        by_x.wait_recv()
        by_b.start()

    def form(*spots):
        places = [(place_of(a, p), p) for a, p in spots]
        for n, _ in places:
            beyond = pack.at[n, 1 - core]
            remote(beyond, beyond, sent.at[0], beside.at[n], row, col_b).wait_recv()
        joint = []
        for n, p in places:
            offset = off_ref[order_ref[p]]
            middle = ((across - offset) & (span - 1)) >= width
            joint.append(
                product(split(jnp.where(middle, pack[n, 0], 0.0)), split(pack[n, 1]))
            )
        for (n, p), joined in zip(places, joint):
            offset = off_ref[order_ref[p]]
            for r in range(0, span, STRIP):
                rows = pl.ds(r, STRIP)
                down_r = r + lax.broadcasted_iota(jnp.int32, (STRIP, span), 0)
                across_r = lax.broadcasted_iota(jnp.int32, (STRIP, span), 1)
                unit = jnp.where(down_r == across_r, 1.0, 0.0)
                row_0, row_1 = down_r >= offset, down_r >= offset + width
                col_0, col_1 = across_r >= offset, across_r >= offset + width
                first, second = pack[n, 0, rows, :], pack[n, 1, rows, :]
                both = joined[r : r + STRIP]
                ahead = jnp.where(col_1, both, first)
                quarters = (
                    jnp.where(row_0 & col_0, ahead, unit),
                    jnp.where(row_0 & jnp.logical_not(col_1), both, 0.0),
                    jnp.where(
                        row_0,
                        jnp.where(jnp.logical_not(row_1) & col_1, second, 0.0),
                        jnp.where(col_0, ahead, 0.0),
                    ),
                    jnp.where(row_1 | col_1, unit, jnp.where(row_0, second, both)),
                )
                for q, quarter in enumerate(quarters):
                    hi, lo = split(quarter)
                    part = pl.ds(q // 2 * span + r, STRIP), pl.ds(q % 2 * span, span)
                    map_hi[n, *part] = hi
                    map_lo[n, *part] = lo

    def form_one(a, p, j):
        form((a, p))

    def form_near(p):
        lines = [line(which, p) for which in (here, over_x, over_y)]
        full = True
        for low, many in lines:
            full = full & (many > 0) & jnp.logical_not(direct(low))

        @pl.when(full)
        def _():
            form(*[(low - begin + p, p) for low, _ in lines])

        skip = jnp.where(full, 1, 0)
        for which in (here, over_x, over_y):
            kind(which, p, only(direct, False, form_one), skip)

    def carry(p, slot):
        return remote(
            state.at[slot], state.at[sweeps - 1 - p], carry_send.at[p], carry_recv.at[p],
            row + 2, col,
        )

    def finish(a, act, keep):
        j = begin + a - (sweeps - 1)
        to_row = lax.div(j, per)
        t = lax.rem(j, per)
        place = pl.ds(side * half, half)

        @pl.when(to_row != row)
        def _():
            act(remote(
                state.at[a], final.at[t, place], last_send.at[a], last_recv.at[t, side],
                to_row, col,
            ))

        if keep:
            @pl.when(to_row == row)
            def _():
                final[t, place, :] = state[a]

    def lasts(u):
        low, high = window(u)
        return (high == sweeps - 1) & (low <= high)

    def passes(u):
        low, high = window(u)
        return (u - STRIDE * low == wide - 1) & (low <= high) & jnp.logical_not(bottom)

    def spills(u):
        p = window(u)[0]
        return passes(u) & (begin + wide - 1 - p == 0) & (p < sweeps - 1)

    def apply(u):
        low, high = window(u)
        tile = begin + u + 1

        @pl.when((u < wide) & (tile < total) & (lax.div(tile, per) != row))
        def _():
            remote(
                state.at[u + sweeps], state.at[u + sweeps], tile_send.at[0, 0],
                tile_recv.at[u + 1], row_x, col,
            ).wait_recv()

        @pl.when(top & (u == 0) & (row != 0))
        def _():
            remote(
                state.at[sweeps - 1], state.at[sweeps - 1], tile_send.at[0, 0],
                tile_recv.at[0], row_x, col,
            ).wait_recv()

        @pl.when((u == STRIDE * high) & (low <= high) & jnp.logical_not(top))
        def _():
            carry(high, sweeps - 1 - high).wait_recv()

        def some(live):
            ready = []
            for i in range(live):
                p = low + i
                a = u - STRIDE * p
                x = jnp.concatenate([state[a - p + sweeps - 1], state[a - p + sweeps]], 1)
                n = place_of(a, p)
                ready.append((a, p, x, map_hi[n], map_lo[n]))
            made = []
            for a, p, x, hi, lo in ready:
                x_hi, x_lo = split(x)
                both = dot(jnp.concatenate([x_hi, x_lo], 0), hi)
                made.append((a, p, both[:half] + (both[half:] + dot(x_hi, lo))))
            for a, p, y in made:
                state[a - p + sweeps - 1] = y[:, :span]
                to = jnp.where(begin + a - p == total - 1, spare, a - p + sweeps)
                state[to] = y[:, span:]

        for live in range(1, most + 1):
            @pl.when(high - low + 1 == live)
            def _(live=live):
                some(live)

        @pl.when(passes(u))
        def _():
            p = window(u)[0]
            carry(p, wide - 1 - p + sweeps).start()

        @pl.when(spills(u))
        def _():
            p = window(u)[0]
            carry(p + 1, wide - 1 - p + sweeps - 1).start()

        @pl.when(lasts(u))
        def _():
            finish(u - STRIDE * (sweeps - 1), lambda c: c.start(), True)

    def over_sweeps(act):
        def one(p, _):
            act(p)
            return 0

        lax.fori_loop(0, sweeps, one, 0)

    def turn(v):
        return v

    def near(v, _):
        @pl.when(v < sweeps)
        def _():
            kind(over_x, turn(v), only(direct, False, relay_x))
            kind(over_y, turn(v), only(direct, False, relay_y))

        p = v - FORM_LAG

        @pl.when(p >= 0)
        def _():
            form_near(turn(p))

        return 0

    def drain_maps(p):
        lines = [line(which, p)[1] for which in (here, over_x, over_y, over_both)]
        straight = [jnp.where(top, jnp.maximum(many - 1, 0), 0) for many in lines]
        turns = jnp.where(onward_x(p), 1, 0)
        total_sends = (
            3 * lines[0] + straight[0] + lines[3]
            + lines[1] + (1 - turns) * (lines[1] - straight[1])
            + lines[2] + turns * (lines[2] - straight[2])
        )
        for k in range(1, 3 * most_lines + 5 * most_lines + 1):
            @pl.when(total_sends == k)
            def _(k=k):
                whole = pack.at[pl.ds(0, k), core]
                remote(whole, whole, sent.at[p], arrive.at[0], row_x, col).wait_send()

    def main(v, _):
        @pl.when(v < sweeps)
        def _():
            kind(over_both, v, close)

            @pl.when(top)
            def _():
                kind(over_x, v, only(direct, True, close))
                kind(over_y, v, only(direct, True, close))

        p = v - FORM_LAG

        @pl.when((p >= 0) & (p < sweeps))
        def _():
            kind(over_both, p, form_one)

            @pl.when(top)
            def _():
                for which in (here, over_x, over_y):
                    kind(which, p, only(direct, True, form_one))

        @pl.when((v == sweeps + FORM_LAG) & (plane > 1))
        def _():
            over_sweeps(drain_maps)

        def one(k, _):
            u = (v - lead) * STRIDE + k

            @pl.when((u >= 0) & (u < steps))
            def _():
                apply(u)

            return 0

        lax.fori_loop(0, STRIDE, one, 0)
        return 0

    def begin_sweeps(low, high):
        for p in range(low, high):
            move(p, lambda c: c.start(), False)

        def one(p, _):
            kind(here, p, only(is_native, True, sow))
            return 0

        lax.fori_loop(low, high, one, 0)

    loads[0].wait()
    loads[1].wait()
    prepare(0, EARLY)
    pl.semaphore_wait(barrier, greeted)
    greet(heard)
    begin_sweeps(0, EARLY)
    prepare(EARLY, sweeps)
    begin_sweeps(EARLY, sweeps)
    loads[2].wait()
    for t in range(per):
        turned[t] = x_ref[pl.ds(t * span, span), :].T

    @pl.when(bottom)
    def _():
        state[total - begin + sweeps - 1] = jnp.zeros((half, span), jnp.float32)


    reach()
    over_sweeps(lambda p: kind(here, p, only(is_native, False, sow)))
    for t in range(per):
        for h in range(2):
            hand_out(t, h, lambda c: c.start(), True)
    lax.fori_loop(0, sweeps + FORM_LAG, near, 0)
    lead = FORM_LAG + jnp.where(top, 0, jnp.where(plane == 1, APPLY_LEAD, sweeps))
    lax.fori_loop(
        0, jnp.maximum(sweeps + FORM_LAG + 1, lax.div(steps + STRIDE - 1, STRIDE) + lead), main, 0
    )

    def drain(u, _):

        @pl.when(passes(u))
        def _():
            p = window(u)[0]
            carry(p, wide - 1 - p + sweeps).wait_send()

        @pl.when(spills(u))
        def _():
            p = window(u)[0]
            carry(p + 1, wide - 1 - p + sweeps - 1).wait_send()

        @pl.when(lasts(u))
        def _():
            finish(u - STRIDE * (sweeps - 1), lambda c: c.wait_send(), False)

        return 0

    lax.fori_loop(0, steps, drain, 0)

    @pl.when(plane <= 1)
    def _():
        over_sweeps(drain_maps)

    for p in range(sweeps):
        move(p, lambda c: c.wait_send(), False)
        move(p, lambda c: c.wait_send(), True)
    for t in range(per):
        for h in range(2):
            hand_out(t, h, lambda c: c.wait_send(), False)
    for t in range(per):
        g = plane_of(row * per + t + sweeps - 1)
        for h in range(2):
            @pl.when(2 * g + h != row)
            def _(t=t, h=h):
                place = final.at[t, pl.ds(h * half, half)]
                remote(
                    place, place, last_send.at[0], last_recv.at[t, h], row_x, col
                ).wait_recv()

        out_ref[pl.ds(t * span, span), :] = final[t].T


def local(rows_n, cols_n, eigvecs, reflectors, factors, order, offsets):
    sweeps, _, span, width = reflectors.shape
    height, columns = eigvecs.shape
    per = height // span
    _, _, _, widest, _, count = shape_of_planes(rows_n, per, sweeps)
    slots = widest + sweeps + 1
    vmem = pl.BlockSpec(memory_space=pltpu.VMEM)
    smem = pl.BlockSpec(memory_space=pltpu.SMEM)
    dma = pltpu.SemaphoreType.DMA
    return pl.pallas_call(
        functools.partial(kernel, rows_n, cols_n),
        out_shape=jax.ShapeDtypeStruct((height, columns), jnp.float32),
        in_specs=[smem, smem] + [pl.BlockSpec(memory_space=pl.ANY)] * 3,
        out_specs=vmem,
        scratch_shapes=[
            pltpu.VMEM((height, columns), jnp.float32),
            pltpu.VMEM((sweeps, 1, width, span), jnp.float32),
            pltpu.VMEM((sweeps, 1, width, width), jnp.float32),
            dma((3,)),
            pltpu.VMEM((count + sweeps, 2, span, span), jnp.float32),
            pltpu.VMEM((count, 2 * span, 2 * span), jnp.bfloat16),
            pltpu.VMEM((count, 2 * span, 2 * span), jnp.bfloat16),
            pltpu.VMEM((slots, columns // 2, span), jnp.float32),
            pltpu.VMEM((per, columns, span), jnp.float32),
            pltpu.VMEM((per, columns, span), jnp.float32),
            dma((count,)),
            dma((count,)),
            dma((sweeps,)),
            dma((sweeps,)),
            dma((per, 2)),
            dma((widest + 1,)),
            dma((sweeps,)),
            dma((sweeps,)),
            dma((widest,)),
            dma((per, 2)),
            pltpu.SemaphoreType.REGULAR,
        ],
        compiler_params=pltpu.CompilerParams(collective_id=0, has_side_effects=True),
    )(order, offsets, eigvecs, jnp.swapaxes(reflectors, 2, 3), factors)


def solution(mesh):
    placed = (
        P("row", "col"),
        P(None, ("row", "col"), None, None),
        P(None, ("row", "col"), None, None),
        P(),
        P(),
    )
    body = functools.partial(local, mesh.shape["row"], mesh.shape["col"])
    return jax.shard_map(
        body, mesh=mesh, in_specs=placed, out_specs=P("row", "col"), check_vma=False
    )
```
